32 devices in a mesh: grp: 2 (over x), dev: 16 (over z, y, core).
Axes of the slice: x: 2, y: 2, z: 4, core: 2. Of those that a mesh axis runs over, the one named last changes fastest.
Arguments:
- inputs: bfloat16 [64, 196, 1024], P(('grp', 'dev')), may hold values from -6 to 6
- cotangent: bfloat16 [64, 196, 1024], P(('grp', 'dev')), may hold values from -6 to 6
- first_gain: float32 [1024], replicated, may hold values from 0.5 to 1.5
- first_shift: float32 [1024], replicated, may hold values from -3 to 3
- token_in: bfloat16 [512, 196], replicated, may hold values from -0.4375 to 0.4375
- token_in_bias: float32 [512], replicated, may hold values from -3 to 3
- token_out: bfloat16 [512, 196], replicated, may hold values from -0.25 to 0.25
- second_gain: float32 [1024], replicated, may hold values from 0.5 to 1.5
- second_shift: float32 [1024], replicated, may hold values from -3 to 3
- channel_in: bfloat16 [1024, 4096], replicated, may hold values from -0.1875 to 0.1875
- channel_in_bias: float32 [4096], replicated, may hold values from -3 to 3
- channel_out: bfloat16 [1024, 4096], replicated, may hold values from -0.09375 to 0.09375
Outputs:
- grad_inputs: bfloat16 [64, 196, 1024], P(('grp', 'dev'))
- grad_token_in: float32 [512, 196], P('dev')
- grad_token_out: float32 [512, 196], P('dev')
- grad_channel_in: float32 [1024, 4096], P('dev')
- grad_channel_out: float32 [1024, 4096], P('dev')
- grad_norms: float32 [5, 1024], replicated
- grad_token_in_bias: float32 [512], replicated
- grad_token_out_bias: float32 [196], replicated
- grad_channel_in_bias: float32 [4096], replicated
The draws below stay inside these ranges and needn't reach their ends.
All inputs are finite; a program needn't handle non-finite values.
Results may differ from the reference program's by a relative error of at most 0.0066.
Values sent between devices are 32-bit elements; how exact they have to be, the bound alone decides.
A program may use at most 192 MiB of HBM per device.

```python
import math
import jax
import jax.numpy as jnp
from jax import lax

P_SIZE = 196
C = 1024
DS = 512
DC = 4096
IMG = 2
BATCH = 64


def spiked(drawn, stream_key, source, target, shards_of, factor):
    def block_of(position):
        return (jnp.arange(drawn.shape[position]) // (drawn.shape[position] // shards_of)).reshape((-1,) + (1,) * (drawn.ndim - 1 - position))

    one_side = jax.random.permutation(stream_key, shards_of)[block_of(target)]
    second = (block_of(target) + shards_of // 2) % shards_of
    return jnp.where((block_of(source) == one_side) | (block_of(source) == second), factor * drawn, drawn)


def levels(key, shape, cuts, least, largest):
    loudness, own = 1.0, jax.random.fold_in(key, 6)
    for position, blocks in cuts:
        heights = jnp.exp(jax.random.uniform(jax.random.fold_in(own, position), (blocks,), jnp.float32, least / len(cuts), largest / len(cuts)))
        loudness = loudness * jnp.repeat(heights, shape[position] // blocks).reshape([-1 if axis == position else 1 for axis in range(len(shape))])
    return loudness


def bell_draw(stream_key, dims, spread, bound, pieces=(), kind=jnp.bfloat16):
    array = spread * jax.random.normal(stream_key, dims, jnp.float32)
    if pieces:
        array = array * levels(stream_key, dims, pieces, -0.22, 0.18)
    return jnp.clip(array, -bound, bound).astype(kind)


def gaussian_with(rng, extent, width, bound, cuts, heavy, kind=jnp.bfloat16):
    array = width * jax.random.normal(rng, extent, jnp.float32)
    if cuts:
        array = array * levels(rng, extent, cuts, -0.22, 0.18)
    return jnp.clip(spiked(array, jax.random.fold_in(rng, 3), *heavy), -bound, bound).astype(kind)


def setup_inputs(seed: int = 0) -> dict:
    key_of = jax.random.split(jax.random.key(seed), 13)
    return {
        "inputs": bell_draw(key_of[0], (BATCH, P_SIZE, C), 1.0, 6.0, ((0, 32),)),
        "cotangent": gaussian_with(key_of[1], (BATCH, P_SIZE, C), 1.0, 6.0, ((0, 32),), (0, 2, 32, 2.75)),
        "first_gain": jnp.clip(jax.random.uniform(key_of[2], (C,), jnp.float32, 0.5, 1.5), 0.5, 1.5),
        "first_shift": bell_draw(key_of[3], (C,), 0.5, 3.0, (), jnp.float32),
        "token_in": bell_draw(key_of[4], (DS, P_SIZE), P_SIZE ** -0.5, 0.4375),
        "token_in_bias": bell_draw(key_of[5], (DS,), 0.5, 3.0, (), jnp.float32),
        "token_out": bell_draw(key_of[6], (DS, P_SIZE), DS ** -0.5, 0.25),
        "second_gain": jnp.clip(jax.random.uniform(key_of[7], (C,), jnp.float32, 0.5, 1.5), 0.5, 1.5),
        "second_shift": bell_draw(key_of[8], (C,), 0.5, 3.0, (), jnp.float32),
        "channel_in": bell_draw(key_of[9], (C, DC), C ** -0.5, 0.1875),
        "channel_in_bias": bell_draw(key_of[10], (DC,), 0.5, 3.0, (), jnp.float32),
        "channel_out": bell_draw(key_of[11], (C, DC), DC ** -0.5, 0.09375),
    }


epsilon = 1e-06

def norm_forward(values, gain, shift):
    centred = values - lax.optimization_barrier(jnp.mean(values, axis=-1, keepdims=True))
    variance = lax.optimization_barrier(jnp.mean(centred * centred, axis=-1, keepdims=True))
    inv_std = lax.rsqrt(variance + epsilon)
    scaled = centred * inv_std
    return (scaled * gain + shift, scaled, inv_std)

def norm_backward(incoming, scaled, inv_std, gain):
    weighted = incoming * gain
    first_mean = lax.optimization_barrier(jnp.mean(weighted, axis=-1, keepdims=True))
    second_mean = lax.optimization_barrier(jnp.mean(weighted * scaled, axis=-1, keepdims=True))
    return inv_std * (weighted - first_mean - scaled * second_mean)

def gelu_value(values):
    return 0.5 * values * (1.0 + lax.erf(values / math.sqrt(2.0)))

def gelu_slope(values):
    return 0.5 * (1.0 + lax.erf(values / math.sqrt(2.0))) + values * jnp.exp(-0.5 * values * values) / math.sqrt(2.0 * math.pi)

def reference(inputs, cotangent, first_gain, first_shift, token_in, token_in_bias, token_out, second_gain, second_shift, channel_in, channel_in_bias, channel_out):
    f32 = jnp.float32
    blocks = BATCH // IMG
    input_blocks = inputs.reshape(blocks, IMG, P_SIZE, C)
    cot_blocks = cotangent.reshape(blocks, IMG, P_SIZE, C)
    token_in_f = token_in.astype(f32)
    token_out_f = token_out.astype(f32)

    def one_block(carry, pair):
        x_block, g_block = pair
        x_float = x_block.astype(f32)
        g_float = g_block.astype(f32)
        normed_one, first_hat, first_rstd = norm_forward(x_float, first_gain, first_shift)
        normed1 = normed_one.astype(jnp.bfloat16)
        hidden1 = jnp.einsum('bpc,sp->bcs', normed1.astype(f32), token_in_f) + token_in_bias
        act1 = gelu_value(hidden1).astype(jnp.bfloat16)
        mixed = x_float + jnp.einsum('bcs,sp->bpc', act1.astype(f32), token_out_f)
        normed_two, second_hat, second_rstd = norm_forward(mixed, second_gain, second_shift)
        normed2 = normed_two.astype(jnp.bfloat16).reshape(-1, C)
        hidden2 = jnp.dot(normed2, channel_in, preferred_element_type=f32) + channel_in_bias
        act2 = gelu_value(hidden2).astype(jnp.bfloat16)
        cot_rows = g_block.reshape(-1, C)
        d_chout = jnp.dot(cot_rows.T, act2, preferred_element_type=f32)
        dact2 = jnp.dot(cot_rows, channel_out, preferred_element_type=f32)
        dhidden2 = (dact2 * gelu_slope(hidden2)).astype(jnp.bfloat16)
        d_chin = jnp.dot(normed2.T, dhidden2, preferred_element_type=f32)
        dnormed2 = jnp.dot(dhidden2, channel_in.T, preferred_element_type=f32).reshape(IMG, P_SIZE, C)
        dmixed = g_float + norm_backward(dnormed2, second_hat, second_rstd, second_gain)
        dmixed_round = dmixed.astype(jnp.bfloat16)
        d_tokout = jnp.einsum('bcs,bpc->sp', act1.astype(f32), dmixed_round.astype(f32))
        dact1 = jnp.einsum('bpc,sp->bcs', dmixed_round.astype(f32), token_out_f)
        dhidden1 = (dact1 * gelu_slope(hidden1)).astype(jnp.bfloat16)
        d_tokin = jnp.einsum('bcs,bpc->sp', dhidden1.astype(f32), normed1.astype(f32))
        dnormed1 = jnp.einsum('bcs,sp->bpc', dhidden1.astype(f32), token_in_f)
        grad_block = (dmixed + norm_backward(dnormed1, first_hat, first_rstd, first_gain)).astype(jnp.bfloat16)
        norms_part = jnp.stack([lax.optimization_barrier(jnp.sum(dnormed1 * first_hat, axis=(0, 1))), lax.optimization_barrier(jnp.sum(dnormed1, axis=(0, 1))), lax.optimization_barrier(jnp.sum(dnormed2 * second_hat, axis=(0, 1))), lax.optimization_barrier(jnp.sum(dnormed2, axis=(0, 1))), lax.optimization_barrier(jnp.sum(g_float, axis=(0, 1)))])
        tb_in = lax.optimization_barrier(jnp.sum(dhidden1.astype(f32), axis=(0, 1)))
        tb_out = lax.optimization_barrier(jnp.sum(dmixed, axis=(0, 2)))
        cb_in = lax.optimization_barrier(jnp.sum(dhidden2.astype(f32), axis=0))
        parts = (d_tokin, d_tokout, d_chin, d_chout, norms_part, tb_in, tb_out, cb_in)
        carry = tuple((a + b for a, b in zip(carry, parts)))
        return (carry, grad_block)
    start = (jnp.zeros((DS, P_SIZE), f32), jnp.zeros((DS, P_SIZE), f32), jnp.zeros((C, DC), f32), jnp.zeros((C, DC), f32), jnp.zeros((5, C), f32), jnp.zeros((DS,), f32), jnp.zeros((P_SIZE,), f32), jnp.zeros((DC,), f32))
    totals, grad_blocks = lax.scan(one_block, start, (input_blocks, cot_blocks))
    grad_inputs = grad_blocks.reshape(BATCH, P_SIZE, C)
    return (grad_inputs, totals[0], totals[1], totals[2], totals[3], totals[4], totals[5], totals[6], totals[7])
```

```python
import functools
import math

import jax
import jax.numpy as jnp
from jax import lax
from jax.sharding import PartitionSpec as P

epsilon = 1e-06


def norm_forward(values, gain, shift):
    centred = values - jnp.mean(values, axis=-1, keepdims=True)
    variance = jnp.mean(centred * centred, axis=-1, keepdims=True)
    inv_std = lax.rsqrt(variance + epsilon)
    scaled = centred * inv_std
    return (scaled * gain + shift, scaled, inv_std)


def norm_backward(incoming, scaled, inv_std, gain):
    weighted = incoming * gain
    first_mean = jnp.mean(weighted, axis=-1, keepdims=True)
    second_mean = jnp.mean(weighted * scaled, axis=-1, keepdims=True)
    return inv_std * (weighted - first_mean - scaled * second_mean)


def gelu_value(values):
    return 0.5 * values * (1.0 + lax.erf(values / math.sqrt(2.0)))


def gelu_slope(values):
    return 0.5 * (1.0 + lax.erf(values / math.sqrt(2.0))) + values * jnp.exp(
        -0.5 * values * values
    ) / math.sqrt(2.0 * math.pi)


SHARES = (9, 11, 12)


def bit_masks(size):
    return [1 << b for b in range(size.bit_length() - 1)]


def cube(mesh_shape):
    masks = bit_masks(mesh_shape["dev"])
    dims = [("dev", masks[0])]
    dims += [("grp", 1 << b) for b in range(mesh_shape["grp"].bit_length() - 1)]
    dims += [("dev", mask) for mask in masks[1:]]
    return dims


def exchange(values, dim, mesh_shape):
    name, mask = dim
    return lax.ppermute(values, name, [(i, i ^ mask) for i in range(mesh_shape[name])])


def relative_rows(rows, dims, mesh_shape):
    groups, devs = mesh_shape["grp"], mesh_shape["dev"]
    inner = rows // (groups * devs)
    index = jnp.arange(rows, dtype=jnp.int32)
    block, offset = index // inner, index % inner
    dev = jnp.full_like(block, lax.axis_index("dev"))
    grp = jnp.full_like(block, lax.axis_index("grp"))
    for place, (name, mask) in enumerate(dims):
        bit = (block >> (len(dims) - 1 - place)) & 1
        if name == "dev":
            dev = dev ^ (bit * mask)
        else:
            grp = grp ^ (bit * mask)
    return (dev * groups + grp) * inner + offset


def row_selector(rows, dims, mesh_shape, kind):
    source = relative_rows(rows, dims, mesh_shape)
    return (source[:, None] == jnp.arange(rows, dtype=jnp.int32)[None, :]).astype(kind)


def take(values, axis, which):
    return lax.index_in_dim(values, which, axis, keepdims=True)


def split(keep, received, axis):
    send, stay = take(keep, axis, 1), take(keep, axis, 0)
    if received is not None:
        send = send + take(received, axis, 1)
        stay = stay + take(received, axis, 0)
    return send, stay


def finish(keep, received):
    total = keep + received
    return total.reshape(total.shape[-2:])


def halve(keep, marks, dims, mesh_shape):
    received = None
    for place in range(len(dims)):
        send, keep = split(keep, received, place)
        send = after(send, marks[place])
        received = exchange(send, dims[place], mesh_shape)
    return finish(keep, received)


def spread(total, mesh_shape):
    groups = mesh_shape["grp"]
    mine = lax.axis_index("grp")
    pieces = [total]
    for step in range(1, groups):
        pieces.append(
            lax.ppermute(total, "grp", [(i, i ^ step) for i in range(groups)])
        )
    rows = []
    for target in range(groups):
        piece = pieces[-1]
        for step in range(groups - 2, -1, -1):
            piece = jnp.where((mine ^ target) == step, pieces[step], piece)
        rows.append(piece)
    return jnp.concatenate(rows, axis=0)


def stage_order(stream, dims):
    first = min(stream + 1, len(dims) - 1)
    return list(range(first, 0, -1)) + list(range(first + 1, len(dims)))


def column_blocks(right):
    unit = right.shape[1] // sum(SHARES)
    blocks, start = [], 0
    for share in SHARES:
        blocks.append(right[:, start : start + share * unit])
        start += share * unit
    return blocks


def after(value, others):
    for other in others:
        corner = other.reshape(-1)[0] if other.ndim == 1 else other[(slice(0, 1),) * other.ndim]
        value = value + 0.0 * corner.reshape(()).astype(value.dtype)
    return value


class Reduction:
    def __init__(self, left, right, dims, mesh_shape):
        self.left, self.blocks = left, column_blocks(right)
        self.dims, self.mesh_shape = dims, mesh_shape
        self.half = left.shape[0] // 2
        self.level = 0
        self.keep = [None] * len(self.blocks)

    def shaped(self, values):
        inner = self.left.shape[0] >> len(self.dims)
        return values.reshape((1,) + (2,) * (len(self.dims) - 1) + (inner, values.shape[1]))

    def product(self, rows, block):
        return jnp.dot(rows, block, preferred_element_type=jnp.float32)

    def open(self):
        sends = [self.product(self.left[self.half :], block) for block in self.blocks]
        self.received = [
            self.shaped(exchange(send, self.dims[0], self.mesh_shape)) for send in sends
        ]
        return sends

    def own(self, stream, place, which):
        rows = take(self.shaped(self.left[: self.half]), place, which)
        product = self.product(rows.reshape(-1, rows.shape[-1]), self.blocks[stream])
        received = take(self.received[stream], place, which)
        return product.reshape(received.shape) + received

    def stage(self):
        sends = []
        for stream in range(len(self.blocks)):
            place = stage_order(stream, self.dims)[self.level]
            if self.level == 0:
                send, stay = self.own(stream, place, 1), self.own(stream, place, 0)
            else:
                send, stay = split(self.keep[stream], self.received[stream], place)
            self.keep[stream] = stay
            self.received[stream] = exchange(send, self.dims[place], self.mesh_shape)
            sends.append(send)
        self.level += 1
        return sends

    def close(self):
        while self.level < len(self.dims) - 1:
            self.stage()
        parts = [finish(k, r) for k, r in zip(self.keep, self.received)]
        return spread(jnp.concatenate(parts, axis=1), self.mesh_shape)


def sum_everywhere(values, marks, dims, mesh_shape):
    for mark, dim in zip(marks, dims):
        values = after(values, mark)
        values = values + exchange(values, dim, mesh_shape)
    return values


def per_device(
    mesh_shape,
    inputs,
    cotangent,
    first_gain,
    first_shift,
    token_in,
    token_in_bias,
    token_out,
    second_gain,
    second_shift,
    channel_in,
    channel_in_bias,
    channel_out,
):
    f32 = jnp.float32
    images, patches, channels = inputs.shape
    x_float = inputs.astype(f32)
    g_float = cotangent.astype(f32)
    normed_one, first_hat, first_rstd = norm_forward(x_float, first_gain, first_shift)
    normed1 = normed_one.astype(jnp.bfloat16)
    hidden1 = (
        jnp.einsum("bpc,sp->bcs", normed1, token_in, preferred_element_type=f32) + token_in_bias
    )
    act1 = gelu_value(hidden1).astype(jnp.bfloat16)
    mixed = x_float + jnp.einsum("bcs,sp->bpc", act1, token_out, preferred_element_type=f32)
    normed_two, second_hat, second_rstd = norm_forward(mixed, second_gain, second_shift)
    normed2 = normed_two.astype(jnp.bfloat16).reshape(-1, channels)
    hidden2 = jnp.dot(normed2, channel_in, preferred_element_type=f32) + channel_in_bias
    act2 = gelu_value(hidden2).astype(jnp.bfloat16)
    cot_rows = cotangent.reshape(-1, channels)
    dims = cube(mesh_shape)
    selector = row_selector(channels, dims, mesh_shape, jnp.bfloat16)
    cot_left = jnp.einsum("rc,tc->rt", selector, cot_rows)
    chout = Reduction(cot_left, act2, dims, mesh_shape)
    opened = chout.open()
    slope_bias = after(channel_in_bias, opened)
    hidden2_again = hidden2 + (slope_bias - channel_in_bias)
    dact2 = jnp.dot(cot_rows, channel_out, preferred_element_type=f32)
    dhidden2 = (dact2 * gelu_slope(hidden2_again)).astype(jnp.bfloat16)
    staged = chout.stage()
    norm_left = after(jnp.einsum("rc,tc->rt", selector, normed2), staged)
    chin = Reduction(norm_left, dhidden2, dims, mesh_shape)
    opened = chin.open()
    dnormed2 = jnp.einsum("tk,ck->tc", dhidden2, channel_in, preferred_element_type=f32).reshape(
        images, patches, channels
    )
    late_gain = after(second_gain, opened)
    dmixed = g_float + norm_backward(dnormed2, second_hat, second_rstd, late_gain)
    dmixed_round = dmixed.astype(jnp.bfloat16)
    dact1 = jnp.einsum("bpc,sp->bcs", dmixed_round, token_out, preferred_element_type=f32)
    dhidden1 = (dact1 * gelu_slope(hidden1)).astype(jnp.bfloat16)
    dnormed1 = jnp.einsum("bcs,sp->bpc", dhidden1, token_in, preferred_element_type=f32)
    grad_inputs = (dmixed + norm_backward(dnormed1, first_hat, first_rstd, first_gain)).astype(
        jnp.bfloat16
    )
    grad_in_piece = jnp.einsum("bcs,bpc->sp", dhidden1, normed1, preferred_element_type=f32)
    grad_out_piece = jnp.einsum("bcs,bpc->sp", act1, dmixed_round, preferred_element_type=f32)
    token_rows = jnp.concatenate([grad_in_piece, grad_out_piece], axis=1)
    hidden_units = token_rows.shape[0]
    token_rows = jnp.dot(
        row_selector(hidden_units, dims, mesh_shape, f32),
        token_rows,
        precision=lax.Precision.HIGHEST,
    )
    token_rows = token_rows.reshape((2,) * len(dims) + (hidden_units >> len(dims), -1))
    chin.stage()
    marks = []
    for level in range(1, len(dims) - 1):
        marks.append(chout.stage())
        marks.append(chin.stage())
    marks = [[]] + [marks[0]] + marks[1::2]
    token_part = spread(halve(token_rows, marks, dims, mesh_shape), mesh_shape)
    chout_part = chout.close()
    chin_part = chin.close()
    norms_part = jnp.stack(
        [
            jnp.sum(dnormed1 * first_hat, axis=(0, 1)),
            jnp.sum(dnormed1, axis=(0, 1)),
            jnp.sum(dnormed2 * second_hat, axis=(0, 1)),
            jnp.sum(dnormed2, axis=(0, 1)),
            jnp.sum(g_float, axis=(0, 1)),
        ]
    )
    tb_in = jnp.sum(dhidden1.astype(f32), axis=(0, 1))
    tb_out = jnp.sum(dmixed, axis=(0, 2))
    cb_in = jnp.sum(dhidden2.astype(f32), axis=0)
    flat = jnp.concatenate([norms_part.reshape(-1), tb_in, tb_out, cb_in])
    edge = -flat.shape[0] % 1024
    flat = jnp.pad(flat, (0, edge)).reshape(-1, 128)
    flat = sum_everywhere(flat, marks, dims, mesh_shape).reshape(-1)
    cuts = [norms_part.size, tb_in.size, tb_out.size, cb_in.size]
    pieces = []
    start = 0
    for size in cuts:
        pieces.append(flat[start : start + size])
        start += size
    norms_total, tb_in_total, tb_out_total, cb_in_total = pieces
    norms_total = norms_total.reshape(norms_part.shape)
    return (
        grad_inputs,
        token_part[:, :patches],
        token_part[:, patches:],
        chin_part,
        chout_part,
        norms_total,
        tb_in_total,
        tb_out_total,
        cb_in_total,
    )


def solution(mesh):
    in_specs = (
        P(("grp", "dev"), None, None),
        P(("grp", "dev"), None, None),
        P(),
        P(),
        P(),
        P(),
        P(),
        P(),
        P(),
        P(),
        P(),
        P(),
    )
    out_specs = (
        P(("grp", "dev"), None, None),
        P("dev", None),
        P("dev", None),
        P("dev", None),
        P("dev", None),
        P(),
        P(),
        P(),
        P(),
    )
    shape = dict(mesh.shape)
    return jax.shard_map(
        functools.partial(per_device, shape), mesh=mesh, in_specs=in_specs, out_specs=out_specs, check_vma=False
    )
```
